256 devices in a mesh: section: 4 (over y_hi, core), dp: 64 (over y_lo, x, z).
Axes of the slice: x: 4, y: 4 (y_hi: 2, y_lo: 2; y = y_hi * 2 + y_lo), z: 8, core: 2. Of those that a mesh axis runs over, the one named last changes fastest.
Arguments:
- section_inputs: bfloat16 [4, 2, 8192, 1024], P('section', None, 'dp'), may hold values from -16 to 16
- gain: float32 [4, 1024], P('section'), may hold values from 0.25 to 1.75
- w_gate: bfloat16 [4, 1024, 1536], P('section'), may hold values from -0.1875 to 0.1875
- w_up: bfloat16 [4, 1024, 1536], P('section'), may hold values from -0.1875 to 0.1875
- w_out: bfloat16 [4, 1024, 1536], P('section'), may hold values from -0.15625 to 0.15625
- out_grad: bfloat16 [2, 8192, 1024], P(None, 'dp'), may hold values from -16 to 16
Outputs:
- grad_w_gate: float32 [4, 1024, 1536], P('section', 'dp')
- grad_w_up: float32 [4, 1024, 1536], P('section', 'dp')
- grad_w_out: float32 [4, 1024, 1536], P('section', 'dp')
- grad_gain: float32 [4, 1024], P('section', 'dp')
- input_grads: bfloat16 [4, 2, 8192, 1024], P('section', None, 'dp')
The draws below stay inside these ranges and needn't reach their ends.
All inputs are finite; a program needn't handle non-finite values.
Results may differ from the reference program's by a relative error of at most 0.014.
Values may be sent and summed in bfloat16 or wider, within the bound.
No kernel may reach another device: no remote copies, remote signals or barrier semaphores. Data moves between devices by JAX's collectives and lax.ppermute only.
A program may use at most 128 MiB of HBM per device.

```python
import jax
import jax.numpy as jnp
from jax import lax

D = 1024
HID = 1536
MICRO = 2
TOK_DEV = 128
TOKENS = 8192
SECTIONS = 4
N_SECTION = 4


def with_spikes(values, own_key, source, target, blocks, factor):
    def block_of(axis_at):
        return (jnp.arange(values.shape[axis_at]) // (values.shape[axis_at] // blocks)).reshape((-1,) + (1,) * (values.ndim - 1 - axis_at))

    one_side = jax.random.permutation(own_key, blocks)[block_of(target)]
    other_side = (block_of(target) + blocks // 2) % blocks
    return jnp.where((block_of(source) == one_side) | (block_of(source) == other_side), factor * values, values)


def block_levels(own_key, dims, pieces, low, largest):
    factor_of, own = 1.0, jax.random.fold_in(own_key, 6)
    for dim, parts in pieces:
        draws = jnp.exp(jax.random.uniform(jax.random.fold_in(own, dim), (parts,), jnp.float32, low / len(pieces), largest / len(pieces)))
        factor_of = factor_of * jnp.repeat(draws, dims[dim] // parts).reshape([-1 if axis == dim else 1 for axis in range(len(dims))])
    return factor_of


def gaussian(own_key, extent, width, limit, shards=(), kind=jnp.bfloat16):
    drawn = width * jax.random.normal(own_key, extent, jnp.float32)
    if shards:
        drawn = drawn * block_levels(own_key, extent, shards, -0.22, 0.18)
    return jnp.clip(drawn, -limit, limit).astype(kind)


def noise_with(rng, shape, scale, reach, split, heavy, dtype=jnp.bfloat16):
    result = scale * jax.random.normal(rng, shape, jnp.float32)
    if split:
        result = result * block_levels(rng, shape, split, -0.22, 0.18)
    return jnp.clip(with_spikes(result, jax.random.fold_in(rng, 3), *heavy), -reach, reach).astype(dtype)


def setup_inputs(seed: int = 0) -> dict:
    seeds = jax.random.split(jax.random.key(seed), 7)
    section_inputs = noise_with(seeds[0], (SECTIONS, MICRO, TOKENS, D), 1.0, 16.0, ((0, 4), (2, 64)), (2, 3, 64, 4.0))
    gain = jnp.clip(1.0 + 0.15 * jax.random.normal(seeds[1], (SECTIONS, D), jnp.float32), 0.25, 1.75)
    w_gate = gaussian(seeds[2], (SECTIONS, D, HID), D ** -0.5, 0.1875, ((0, 4),))
    w_up = gaussian(seeds[3], (SECTIONS, D, HID), D ** -0.5, 0.1875, ((0, 4),))
    w_out = gaussian(seeds[4], (SECTIONS, D, HID), HID ** -0.5, 0.15625, ((0, 4),))
    out_grad = noise_with(seeds[5], (MICRO, TOKENS, D), 1.0, 16.0, ((1, 64),), (1, 2, 64, 4.0))
    return {"section_inputs": section_inputs, "gain": gain, "w_gate": w_gate, "w_up": w_up, "w_out": w_out, "out_grad": out_grad}


C_GELU = 0.7978845608028654
EPSILON = 1e-06

def gelu_parts(pre_act):
    cubic = 0.044715 * pre_act * pre_act * pre_act
    tangent = jnp.tanh(C_GELU * (pre_act + cubic))
    gelu_value = 0.5 * pre_act * (1.0 + tangent)
    gelu_slope = 0.5 * (1.0 + tangent) + 0.5 * pre_act * (1.0 - tangent * tangent) * C_GELU * (1.0 + 3.0 * 0.044715 * pre_act * pre_act)
    return (gelu_value, gelu_slope)

def section_back(inputs_row, incoming, gain_row, w_gate_mat, w_up_mat, w_out_mat):
    inputs_float = inputs_row.astype(jnp.float32)
    inverse_rms = lax.rsqrt(lax.optimization_barrier(jnp.mean(inputs_float * inputs_float, axis=-1, keepdims=True)) + EPSILON)
    normed = (inputs_float * inverse_rms * gain_row).astype(jnp.bfloat16)
    gate_pre = jnp.dot(normed, w_gate_mat, preferred_element_type=jnp.float32)
    up_pre = jnp.dot(normed, w_up_mat, preferred_element_type=jnp.float32)
    gelu_value, gelu_slope = gelu_parts(gate_pre)
    hidden_act = (gelu_value * up_pre).astype(jnp.bfloat16)
    act_grad = jnp.dot(incoming, w_out_mat, preferred_element_type=jnp.float32)
    gate_grad = (act_grad * up_pre * gelu_slope).astype(jnp.bfloat16)
    up_grad = (act_grad * gelu_value).astype(jnp.bfloat16)
    transpose_dims = (((1,), (1,)), ((), ()))
    normed_grad = lax.dot_general(gate_grad, w_gate_mat, transpose_dims, preferred_element_type=jnp.float32)
    normed_grad = normed_grad + lax.dot_general(up_grad, w_up_mat, transpose_dims, preferred_element_type=jnp.float32)
    gain_term = lax.optimization_barrier(jnp.sum(normed_grad * inputs_float * inverse_rms, axis=0))
    scaled_grad = normed_grad * gain_row
    input_grad = inverse_rms * scaled_grad - inputs_float * inverse_rms ** 3 * lax.optimization_barrier(jnp.mean(scaled_grad * inputs_float, axis=-1, keepdims=True))
    passed = (incoming.astype(jnp.float32) + input_grad).astype(jnp.bfloat16)
    return (passed, hidden_act, gate_grad, up_grad, normed, gain_term)

def reference(section_inputs, gain, w_gate, w_up, w_out, out_grad):
    token_scale = 1.0 / (MICRO * TOK_DEV)
    contract = (((0,), (0,)), ((), ()))
    grads_gate = []
    grads_up = []
    grads_out = []
    grads_gain = []
    passed_all = []
    incoming_all = out_grad
    for section_level in reversed(range(N_SECTION)):
        gate_sum = jnp.zeros((D, HID), jnp.float32)
        up_sum = jnp.zeros((D, HID), jnp.float32)
        out_sum = jnp.zeros((D, HID), jnp.float32)
        gain_sum = jnp.zeros((D,), jnp.float32)
        passed_list = []
        for member in range(MICRO):
            incoming = incoming_all[member]
            passed, hidden_act, gate_grad, up_grad, normed, gain_term = section_back(section_inputs[section_level, member], incoming, gain[section_level], w_gate[section_level], w_up[section_level], w_out[section_level])
            gate_sum = gate_sum + lax.dot_general(normed, gate_grad, contract, preferred_element_type=jnp.float32)
            up_sum = up_sum + lax.dot_general(normed, up_grad, contract, preferred_element_type=jnp.float32)
            out_sum = out_sum + lax.dot_general(incoming, hidden_act, contract, preferred_element_type=jnp.float32)
            gain_sum = gain_sum + gain_term
            passed_list.append(passed)
        incoming_all = jnp.stack(passed_list)
        passed_all.append(incoming_all)
        grads_gate.append(gate_sum * token_scale)
        grads_up.append(up_sum * token_scale)
        grads_out.append(out_sum * token_scale)
        grads_gain.append(gain_sum * token_scale)
    return (jnp.stack(grads_gate[::-1]), jnp.stack(grads_up[::-1]), jnp.stack(grads_out[::-1]), jnp.stack(grads_gain[::-1]), jnp.stack(passed_all[::-1]))
```

```python
import jax
import jax.numpy as jnp
from jax import lax
from jax.experimental import pallas as pl
from jax.experimental.pallas import tpu as pltpu
from jax.sharding import Mesh
from jax.sharding import PartitionSpec as P

C_GELU = 0.7978845608028654
EPSILON = 1e-06
BLOCK = 256
BF16 = jnp.bfloat16
F32 = jnp.float32
DP = ("y", "x", "z")
VMEM_LIMIT = 48 * 1024 * 1024


def whole(shape):
    return pl.BlockSpec(shape, lambda *_: (0,) * len(shape))


def params():
    return pltpu.CompilerParams(
        dimension_semantics=("arbitrary",), vmem_limit_bytes=VMEM_LIMIT
    )


def inverse_rms_of(rows):
    return lax.rsqrt(jnp.mean(rows * rows, axis=-1, keepdims=True) + EPSILON)


def gelu_parts(pre_act):
    squared = pre_act * pre_act
    tangent = jnp.tanh(C_GELU * (pre_act + 0.044715 * squared * pre_act))
    half_open = 0.5 * (1.0 + tangent)
    slope = half_open + 0.5 * pre_act * (1.0 - tangent * tangent) * C_GELU * (
        1.0 + 3.0 * 0.044715 * squared
    )
    return (pre_act * half_open, slope)


def pre_kernel(x_ref, gain_ref, gate_ref, up_ref, normed_ref, hidden_ref, a_ref, b_ref):
    @pl.when(pl.program_id(0) == 0)
    def _():
        rows = x_ref[...].astype(F32)
        normed_ref[...] = (rows * inverse_rms_of(rows) * gain_ref[...]).astype(BF16)

    normed = normed_ref[...]
    gate_pre = jnp.dot(normed, gate_ref[...], preferred_element_type=F32)
    up_pre = jnp.dot(normed, up_ref[...], preferred_element_type=F32)
    value, slope = gelu_parts(gate_pre)
    hidden_ref[...] = (value * up_pre).astype(BF16)
    a_ref[...] = (up_pre * slope).astype(BF16)
    b_ref[...] = value.astype(BF16)


def pre(rows, gain_row, w_gate, w_up):
    count, width = rows.shape
    hid = w_gate.shape[1]
    column = lambda n: pl.BlockSpec((n, BLOCK), lambda j: (0, j))
    return pl.pallas_call(
        pre_kernel,
        grid=(hid // BLOCK,),
        in_specs=[whole((count, width)), whole((1, width)), column(width), column(width)],
        out_specs=[whole((count, width)), column(count), column(count), column(count)],
        out_shape=[jax.ShapeDtypeStruct((count, width), BF16)]
        + [jax.ShapeDtypeStruct((count, hid), BF16)] * 3,
        compiler_params=params(),
        cost_estimate=pl.CostEstimate(
            flops=4 * count * width * hid,
            bytes_accessed=4 * width * hid + 4 * count * width + 6 * count * hid,
            transcendentals=count * hid,
        ),
        name="pre",
    )(rows, gain_row, w_gate, w_up)


def tick_kernel(g_ref, x_ref, gain_ref, a_ref, b_ref, out_ref, gate_ref, up_ref, passed_ref, acc_ref):
    step = pl.program_id(0)
    act = jnp.dot(g_ref[...], out_ref[...], preferred_element_type=F32)
    gate_grad = (act * a_ref[...].astype(F32)).astype(BF16)
    up_grad = (act * b_ref[...].astype(F32)).astype(BF16)
    across = (((1,), (1,)), ((), ()))
    part = lax.dot_general(gate_grad, gate_ref[...], across, preferred_element_type=F32)
    part = part + lax.dot_general(up_grad, up_ref[...], across, preferred_element_type=F32)

    @pl.when(step == 0)
    def _():
        acc_ref[...] = part

    @pl.when(step > 0)
    def _():
        acc_ref[...] += part

    @pl.when(step == pl.num_programs(0) - 1)
    def _():
        rows = x_ref[...].astype(F32)
        inverse_rms = inverse_rms_of(rows)
        scaled = acc_ref[...] * gain_ref[...]
        mean = jnp.mean(scaled * rows, axis=-1, keepdims=True)
        grad = inverse_rms * scaled - rows * (inverse_rms * inverse_rms * inverse_rms * mean)
        passed_ref[...] = (g_ref[...].astype(F32) + grad).astype(BF16)


def tick(g, rows, micro, gain_row, a, b, w_out, w_gate, w_up):
    count, width = g.shape
    hid = w_gate.shape[1]
    weight = pl.BlockSpec((width, BLOCK), lambda j: (0, j))
    saved = pl.BlockSpec((count, BLOCK), lambda j: (micro, j))
    return pl.pallas_call(
        tick_kernel,
        grid=(hid // BLOCK,),
        in_specs=[
            whole((count, width)),
            pl.BlockSpec((count, width), lambda j: (micro, 0)),
            whole((1, width)),
            saved,
            saved,
            weight,
            weight,
            weight,
        ],
        out_specs=whole((count, width)),
        out_shape=jax.ShapeDtypeStruct((count, width), BF16),
        scratch_shapes=[pltpu.VMEM((count, width), F32)],
        compiler_params=params(),
        cost_estimate=pl.CostEstimate(
            flops=6 * count * width * hid, bytes_accessed=6 * width * hid, transcendentals=0
        ),
        name="tick",
    )(g, rows, gain_row, a, b, w_out, w_gate, w_up)


def weights_kernel(first, second):
    def kernel(
        place_ref, g0_ref, g1_ref, g2_ref, g3_ref, n_own_ref, n_pair_ref, h_own_ref, h_pair_ref,
        a_own_ref, a_pair_ref, b_own_ref, b_pair_ref, out_ref, send_ref, keep_ref,
        g_ref, tall_ref, nt_ref, gt_ref,
    ):
        quarter = g0_ref.shape[0]
        tokens, width = g_ref.shape
        half = width // 2
        slot = half // 4
        owner = slot // 8

        @pl.when(pl.program_id(0) == 0)
        def _():
            y, x, z = place_ref[0], place_ref[1], place_ref[2]
            for k, ref in enumerate((g0_ref, g1_ref, g2_ref, g3_ref)):
                g_ref[k * quarter : (k + 1) * quarter, :] = ref[...]

            def arrange(pick, target_ref):
                lower, upper = pick(slice(0, half)), pick(slice(half, width))
                mine = jnp.where(y == 0, lower.astype(F32), upper.astype(F32))
                tall_ref[...] = mine.T.astype(BF16)
                for k, mask in enumerate((first, first ^ second, 0, second)):
                    chunk = (x ^ mask) * slot
                    for d in range(8):
                        source = chunk + ((z + d) & 7) * owner
                        source = pl.multiple_of(source, owner)
                        start = k * slot + d * owner
                        target_ref[start : start + owner, :] = tall_ref[pl.ds(source, owner), :]

            arrange(lambda s: g_ref[:, s], gt_ref)
            arrange(lambda s: jnp.concatenate([n_own_ref[:, s], n_pair_ref[:, s]], axis=0), nt_ref)

        both = lambda one, other: jnp.concatenate([one[...], other[...]], axis=0)
        act = jnp.dot(g_ref[...], out_ref[...], preferred_element_type=F32)
        gate_grad = (act * both(a_own_ref, a_pair_ref).astype(F32)).astype(BF16)
        up_grad = (act * both(b_own_ref, b_pair_ref).astype(F32)).astype(BF16)
        hidden = both(h_own_ref, h_pair_ref)
        for t, (left_ref, right) in enumerate(
            ((nt_ref, gate_grad), (nt_ref, up_grad), (gt_ref, hidden))
        ):
            part = jnp.dot(left_ref[...], right, preferred_element_type=F32) * (1.0 / (2 * quarter))
            part = part.astype(BF16)
            for k in range(2):
                send_ref[t, k] = part[k * slot : (k + 1) * slot]
                keep_ref[t, k] = part[(k + 2) * slot : (k + 3) * slot]

    return kernel


def weight_grads(colour, masks, place, grads, normed, hidden, a, b, w_out):
    quarter, width = grads[0].shape
    hid = w_out.shape[1]
    steps = hid // BLOCK // 2
    tokens = 4 * quarter
    slot = width // 8
    full = lambda shape: pl.BlockSpec(shape, lambda j, _: (0,) * len(shape))
    saved = pl.BlockSpec((tokens // 2, BLOCK), lambda j, _: (0, colour * steps + j))
    piece = pl.BlockSpec((3, 2, slot, BLOCK), lambda j, _: (0, 0, 0, j))
    result = jax.ShapeDtypeStruct((3, 2, slot, hid // 2), BF16)
    return pl.pallas_call(
        weights_kernel(*masks),
        grid_spec=pltpu.PrefetchScalarGridSpec(
            num_scalar_prefetch=1,
            grid=(steps,),
            in_specs=[full((quarter, width))] * 4
            + [full((tokens // 2, width))] * 2
            + [saved] * 6
            + [pl.BlockSpec((width, BLOCK), lambda j, _: (0, colour * steps + j))],
            out_specs=[piece, piece],
            scratch_shapes=[
                pltpu.VMEM((tokens, width), BF16),
                pltpu.VMEM((width // 2, tokens), BF16),
                pltpu.VMEM((width // 2, tokens), BF16),
                pltpu.VMEM((width // 2, tokens), BF16),
            ],
        ),
        out_shape=[result, result],
        compiler_params=params(),
        cost_estimate=pl.CostEstimate(
            flops=5 * tokens * width * hid // 2,
            bytes_accessed=4 * width * hid + 6 * tokens * hid,
            transcendentals=0,
        ),
        name="weight_grads",
    )(place, *grads, *normed, *hidden, *a, *b, w_out)


def after(value, *others):
    return lax.optimization_barrier((value, *others))[0]


def local(section_inputs, gain, w_gate, w_up, w_out, out_grad):
    position = lax.axis_index("section")
    place = jnp.stack([lax.axis_index(a) for a in DP]).astype(jnp.int32)
    w_gate, w_up, w_out = w_gate[0], w_up[0], w_out[0]
    micro_count, tok_rows, width = section_inputs.shape[1:]
    hid = w_gate.shape[1]
    rows = section_inputs[0].reshape(micro_count * tok_rows, width)
    micros = range(micro_count)

    swap = [(0, 1), (1, 0)]
    rows_pair = lax.ppermute(rows, "y", swap)
    loss_pair = lax.ppermute(out_grad, ("section", "y"), [(6, 7), (7, 6)])
    normed, hidden, a, b = pre(rows, gain, w_gate, w_up)

    def run(section, micro, g, held):
        return lax.cond(
            position == section,
            lambda: tick(g, rows, micro, gain, a, b, w_out, w_gate, w_up),
            lambda: held,
        )

    def hop(value, section, crossed):
        pairs = [(2 * (section + 1) + y, 2 * section + (y ^ crossed)) for y in range(2)]
        return lax.ppermute(value, ("section", "y"), pairs)

    passed = [run(3, m, out_grad[m], out_grad[m]) for m in micros]
    rows_pair = after(rows_pair, passed[1])
    normed_pair, hidden_pair, a_pair, b_pair = pre(rows_pair, gain, w_gate, w_up)
    own = [out_grad[m] for m in micros]
    pair = [loss_pair[m] for m in micros]
    for section in (2, 1, 0):
        here = position == section
        arrived = [hop(passed[m], section, 0) for m in micros]
        if section == 1:
            crossed = [
                lax.ppermute(arrived[m], ("section", "y"), [(2, 3), (3, 2)]) for m in micros
            ]
        else:
            crossed = [hop(passed[m], section, 1) for m in micros]
        own = [jnp.where(here, arrived[m], own[m]) for m in micros]
        pair = [jnp.where(here, crossed[m], pair[m]) for m in micros]
        if section:
            passed = [run(section, m, arrived[m], passed[m]) for m in micros]

    masks = ((1, 3), (3, 1))
    parts = [
        weight_grads(
            colour, masks[colour], place, (*own, *pair), (normed, normed_pair),
            (hidden, hidden_pair), (a, a_pair), (b, b_pair), w_out,
        )
        for colour in range(2)
    ]
    late = [after(arrived[0], parts[0][0]), after(arrived[1], parts[1][0])]
    passed = [run(0, m, late[m], passed[m]) for m in micros]

    summed = []
    for colour in range(2):
        first, second = masks[colour]
        to = lambda mask: [(i, i ^ mask) for i in range(4)]
        send, keep = parts[colour]
        keep = keep + lax.ppermute(send, "x", to(first))
        got = lax.ppermute(keep[:, 1], "x", to(second))
        summed.append(keep[:, 0] + got)
    summed = jnp.stack(summed)
    owned = summed.shape[2] // 8
    pieces = [summed[:, :, d * owned : (d + 1) * owned] for d in range(8)]
    total = pieces[0].astype(F32)
    for d in range(1, 8):
        got = lax.ppermute(pieces[d], "z", [(i, (i + d) % 8) for i in range(8)])
        total = total + got.astype(F32)
    grad_gate, grad_up, grad_out = [
        jnp.concatenate([total[0, t], total[1, t]], axis=-1) for t in range(3)
    ]
    start = lax.axis_index(DP) * owned
    mine = lambda w: lax.dynamic_slice_in_dim(w, start, owned, 0).astype(F32)
    dots = jnp.sum(mine(w_gate) * grad_gate + mine(w_up) * grad_up, axis=-1)
    grad_gain = dots / lax.dynamic_slice_in_dim(gain[0], start, owned, 0)
    return (
        grad_gate[None],
        grad_up[None],
        grad_out[None],
        grad_gain[None],
        jnp.stack(passed)[None],
    )


def solution(mesh):
    torus = Mesh(mesh.devices.reshape(4, 2, 4, 8), ("section", *DP))
    return jax.shard_map(
        local,
        mesh=torus,
        in_specs=(
            P("section", None, DP, None),
            P("section", None),
            P("section", None, None),
            P("section", None, None),
            P("section", None, None),
            P(None, DP, None),
        ),
        out_specs=(
            P("section", DP, None),
            P("section", DP, None),
            P("section", DP, None),
            P("section", DP),
            P("section", None, DP, None),
        ),
        check_vma=False,
    )
```
